64 devices in a mesh: dp: 4 (over x, y), sp: 16 (over z, core).
Axes of the slice: x: 2, y: 2, z: 8, core: 2. Of those that a mesh axis runs over, the one named last changes fastest.
The devices are a block of a 4x4x8 slice.
Arguments:
- images: float32 [32, 256, 256, 3], P('dp', 'sp'), parts along dimension 0
- w_patch: bfloat16 [16, 16, 3, 768], replicated
- b_patch: float32 [768], replicated
- pos_embed: bfloat16 [256, 768], P('sp')
- ln1_gain: float32 [768], replicated
- ln1_bias: float32 [768], replicated
- w_qkv: bfloat16 [768, 3, 12, 64], replicated
- b_qkv: float32 [3, 12, 64], replicated
- w_out: bfloat16 [12, 64, 768], replicated
- b_out: float32 [768], replicated
- ln2_gain: float32 [768], replicated
- ln2_bias: float32 [768], replicated
- w_fc1: bfloat16 [768, 3072], replicated
- b_fc1: float32 [3072], replicated
- w_fc2: bfloat16 [3072, 768], replicated
- b_fc2: float32 [768], replicated
Outputs:
- output: bfloat16 [32, 256, 768], P('dp', 'sp'), parts along dimension 0
There are 4 independent parts. The reference program is written for one: setup_inputs(seed, part) draws one part's arguments, and reference() takes and returns one part's arrays. A program takes and returns all parts, laid end to end along the dimension named above; an argument that names none is the same for every part.
All inputs are finite; a program needn't handle non-finite values.
Results may differ from the reference program's by a relative error of at most 0.0126143.
Values are sent between devices in bfloat16 or wider.
A program may use at most 768 MiB of HBM per device.

```python
import jax
import jax.numpy as jnp
from jax import lax

B = 8
IMG = 256
PATCH = 16
D = 768
HEADS = 12
HEAD = 64
FF = 3072

GRID = IMG // PATCH
TOKENS = GRID * GRID
PATCH_DIM = PATCH * PATCH * 3
LN_EPS = 1e-6


def draw_normal(rng_key, arr_shape, std_dev):
    return jax.random.normal(rng_key, arr_shape, jnp.float32) * std_dev


def smooth_images(base_key, num_images):
    key_freq, key_phase, key_amp, key_noise = jax.random.split(base_key, 4)
    wave_freq = jax.random.uniform(key_freq, (num_images, 8, 2), jnp.float32, -4.0, 4.0) * (2.0 * jnp.pi / IMG)
    wave_phase = jax.random.uniform(key_phase, (num_images, 8, 3), jnp.float32, 0.0, 2.0 * jnp.pi)
    wave_amp = draw_normal(key_amp, (num_images, 8, 3), 0.5)
    coords = jnp.arange(IMG, dtype=jnp.float32)
    row_angle = wave_freq[:, :, 0, None] * coords
    col_angle = wave_freq[:, :, 1, None, None] * coords[:, None] + wave_phase[:, :, None, :]
    waves = (jnp.einsum('nky,nkxc->nyxc', jnp.cos(row_angle), wave_amp[:, :, None, :] * jnp.cos(col_angle))
             - jnp.einsum('nky,nkxc->nyxc', jnp.sin(row_angle), wave_amp[:, :, None, :] * jnp.sin(col_angle)))
    return waves + draw_normal(key_noise, (num_images, IMG, IMG, 3), 0.2)


def setup_inputs(seed: int = 0, part: int = 0) -> dict:
    sub_keys = jax.random.split(jax.random.key(seed), 16)
    qk_gain = jnp.array([1.5, 1.5, 1.0], jnp.float32)[None, :, None, None]
    return {
        'images': smooth_images(jax.random.fold_in(sub_keys[0], part), B),
        'w_patch': draw_normal(sub_keys[1], (PATCH, PATCH, 3, D), PATCH_DIM ** -0.5).astype(jnp.bfloat16),
        'b_patch': draw_normal(sub_keys[2], (D,), 0.5),
        'pos_embed': draw_normal(sub_keys[3], (TOKENS, D), 1.0).astype(jnp.bfloat16),
        'ln1_gain': 1.0 + draw_normal(sub_keys[4], (D,), 0.2),
        'ln1_bias': draw_normal(sub_keys[5], (D,), 0.5),
        'w_qkv': (draw_normal(sub_keys[6], (D, 3, HEADS, HEAD), D ** -0.5) * qk_gain).astype(jnp.bfloat16),
        'b_qkv': draw_normal(sub_keys[7], (3, HEADS, HEAD), 0.5),
        'w_out': draw_normal(sub_keys[8], (HEADS, HEAD, D), 2.0 * D ** -0.5).astype(jnp.bfloat16),
        'b_out': draw_normal(sub_keys[9], (D,), 0.5),
        'ln2_gain': 1.0 + draw_normal(sub_keys[10], (D,), 0.2),
        'ln2_bias': draw_normal(sub_keys[11], (D,), 0.5),
        'w_fc1': draw_normal(sub_keys[12], (D, FF), D ** -0.5).astype(jnp.bfloat16),
        'b_fc1': draw_normal(sub_keys[13], (FF,), 0.5),
        'w_fc2': draw_normal(sub_keys[14], (FF, D), 1.5 * FF ** -0.5).astype(jnp.bfloat16),
        'b_fc2': draw_normal(sub_keys[15], (D,), 0.5),
    }


def layer_norm(x_in, ln_gain, ln_bias):
    row_mean = jnp.mean(x_in, axis=-1, keepdims=True)
    centered = x_in - row_mean
    variance = jnp.mean(centered * centered, axis=-1, keepdims=True)
    return centered * lax.rsqrt(variance + LN_EPS) * ln_gain + ln_bias


def reference(images, w_patch, b_patch, pos_embed, ln1_gain, ln1_bias, w_qkv, b_qkv, w_out, b_out, ln2_gain, ln2_bias, w_fc1, b_fc1, w_fc2, b_fc2):
    w_patch_flat = w_patch.reshape(PATCH_DIM, D)
    w_qkv_flat = w_qkv.reshape(D, 3 * D)
    b_qkv_flat = b_qkv.reshape(3 * D)
    w_out_flat = w_out.reshape(D, D)
    pos_f32 = pos_embed.astype(jnp.float32)

    def encode_image(single_image):
        pixels = single_image.astype(jnp.bfloat16).reshape(GRID, PATCH, GRID, PATCH, 3)
        patches = jnp.transpose(pixels, (0, 2, 1, 3, 4)).reshape(TOKENS, PATCH_DIM)
        patch_embed = jnp.dot(patches, w_patch_flat, preferred_element_type=jnp.float32)
        x_zero = (patch_embed + b_patch + pos_f32).astype(jnp.bfloat16)
        normed = layer_norm(x_zero.astype(jnp.float32), ln1_gain, ln1_bias).astype(jnp.bfloat16)
        qkv_proj = (jnp.dot(normed, w_qkv_flat, preferred_element_type=jnp.float32) + b_qkv_flat).astype(jnp.bfloat16)
        queries = qkv_proj[:, :D].reshape(GRID, GRID, HEADS, HEAD)
        keys_all = qkv_proj[:, D:2 * D].reshape(TOKENS, HEADS, HEAD).astype(jnp.float32)
        values_all = qkv_proj[:, 2 * D:].reshape(TOKENS, HEADS, HEAD).astype(jnp.float32)

        def attend_row(row_queries):
            scores = jnp.einsum('qhe,khe->hqk', row_queries.astype(jnp.float32), keys_all) * HEAD ** -0.5
            weights = jax.nn.softmax(scores, axis=-1).astype(jnp.bfloat16).astype(jnp.float32)
            return jnp.einsum('hqk,khe->qhe', weights, values_all).astype(jnp.bfloat16)

        attended = lax.map(attend_row, queries).reshape(TOKENS, D)
        residual = x_zero.astype(jnp.float32) + jnp.dot(attended, w_out_flat, preferred_element_type=jnp.float32) + b_out
        normed_two = layer_norm(residual, ln2_gain, ln2_bias).astype(jnp.bfloat16)
        hidden = jax.nn.gelu(jnp.dot(normed_two, w_fc1, preferred_element_type=jnp.float32) + b_fc1, approximate=True).astype(jnp.bfloat16)
        return (residual + jnp.dot(hidden, w_fc2, preferred_element_type=jnp.float32) + b_fc2).astype(jnp.bfloat16)

    return lax.map(encode_image, images)
```

```python
import functools
import math

import jax
import jax.numpy as jnp
from jax import lax
from jax.experimental import pallas as pl
from jax.experimental.pallas import tpu as pltpu
from jax.sharding import PartitionSpec as P

MESH = pl.DeviceIdType.MESH
LN_EPS = 1e-6
F32 = jnp.float32
BF16 = jnp.bfloat16


def dot(a, b, rhs_t=False):
    dims = (((1,), (1 if rhs_t else 0,)), ((), ()))
    return lax.dot_general(a, b, dims, preferred_element_type=F32)


def layer_norm(z, gain, bias):
    mean = jnp.mean(z, axis=-1, keepdims=True)
    centered = z - mean
    var = jnp.mean(centered * centered, axis=-1, keepdims=True)
    return centered * lax.rsqrt(var + LN_EPS) * gain + bias


def gelu_tanh(v):
    return 0.5 * v * (1.0 + jnp.tanh(math.sqrt(2.0 / math.pi) * (v + 0.044715 * (v * v * v))))


def kernel(cfg, img_hbm, wp_hbm, bp_hbm, pos_hbm, g1_hbm, b1_hbm, wqkv_hbm, bqkv_hbm, wo_hbm, bo_hbm, g2_hbm, c2_hbm,
           w1_hbm, bf1_hbm, w2_hbm, bf2_hbm, out_ref,
           img, wp, bp, pos, g1, b1, wqkv, bqkv, wo, bo, g2, c2, w1, bf1, w2, bf2,
           lhs, sel, x0h, x0r, bq, qb, kb, vb, ob, orx, acc,
           dsem, xs, xr, ks, kr, os_, or_):
    NZ, T, PL, C, D, H, HD, FF, NG = cfg
    me = lax.axis_index("sp")
    core = lax.rem(me, 2)
    z = lax.div(me, 2)
    partner = me + 1 - 2 * core
    ROWS = NZ * T

    def peer(t):
        return lax.rem(z + t + NZ, NZ) * 2 + core

    barrier = pltpu.get_barrier_semaphore()
    for t in range(1, NZ):
        pl.semaphore_signal(barrier, inc=1, device_id={"sp": peer(t)}, device_id_type=MESH)
    pl.semaphore_signal(barrier, inc=1, device_id={"sp": partner}, device_id_type=MESH)

    first = [(img_hbm, img), (wp_hbm.at[:, 0], wp.at[0]), (wp_hbm.at[:, 1], wp.at[1]), (wp_hbm.at[:, 2], wp.at[2]),
             (bp_hbm, bp), (pos_hbm, pos)]
    later = [(g1_hbm, g1), (b1_hbm, b1), (wqkv_hbm, wqkv), (bqkv_hbm, bqkv), (wo_hbm, wo), (bo_hbm, bo),
             (g2_hbm, g2), (c2_hbm, c2), (w1_hbm, w1), (bf1_hbm, bf1), (w2_hbm, w2), (bf2_hbm, bf2)]
    cps = [pltpu.make_async_copy(s, d, dsem.at[i]) for i, (s, d) in enumerate(first + later)]
    first_c, later_c = cps[:len(first)], cps[len(first):]
    for c in first_c:
        c.start()

    r = lax.broadcasted_iota(jnp.int32, (256, 256), 0)
    cc = lax.broadcasted_iota(jnp.int32, (256, 256), 1)
    same_q = lax.rem(r, 16) == lax.rem(cc, 16)
    for pp in range(PL // 2):
        hit = same_q & (lax.div(cc, 16) == 2 * pp + lax.div(r, 128))
        sel[pp * 256:(pp + 1) * 256, :] = jnp.where(hit, 1.0, 0.0).astype(BF16)

    first_c[0].wait()
    for c in later_c:
        c.start()

    m8 = lax.div(lax.broadcasted_iota(jnp.int32, (8, 128), 1), 16) == lax.broadcasted_iota(jnp.int32, (8, 128), 0)

    def spread(t, carry):
        b = lax.rem(z + t, NZ)
        for c in range(C):
            for p in range(PL):
                row = img[b, c, p:p + 1, :]
                lo = jnp.where(m8, jnp.broadcast_to(row[:, :128], (8, 128)), 0.0)
                hi = jnp.where(m8, jnp.broadcast_to(row[:, 128:], (8, 128)), 0.0)
                at = pl.multiple_of(c * ROWS + t * 16, 16)
                lhs[pl.ds(at, 16), p * 128:(p + 1) * 128] = jnp.concatenate([lo, hi], axis=0).astype(BF16)
        return carry

    lax.fori_loop(0, NZ, spread, 0)
    xsel = dot(lhs[...], sel[...]).astype(BF16)
    for c in first_c[1:]:
        c.wait()
    x0 = jnp.zeros((ROWS, D), F32)
    for c in range(C):
        x0 = x0 + dot(xsel[c * ROWS:(c + 1) * ROWS], wp[c].reshape(PL * 16, D))
    posb = jnp.broadcast_to(pos[...].astype(F32)[None], (NZ, T, D)).reshape(ROWS, D)
    x0 = (x0 + bp[...].reshape(1, D) + posb).astype(BF16)
    x0h[...] = x0
    x0r[0:T, :] = x0[0:T]

    pl.semaphore_wait(barrier, NZ)
    order = sorted(range(1, NZ), key=lambda t: -min(t, NZ - t))
    sends = []
    for t in order:
        cp = pltpu.make_async_remote_copy(src_ref=x0h.at[t * T:(t + 1) * T], dst_ref=x0r.at[t * T:(t + 1) * T],
                                          send_sem=xs.at[t], recv_sem=xr.at[t], device_id={"sp": peer(t)}, device_id_type=MESH)
        cp.start()
        sends.append(cp)

    for c in later_c[:4]:
        c.wait()
    for t3 in range(3):
        for h in range(H):
            bq[0:1, t3 * D + h * HD:t3 * D + (h + 1) * HD] = bqkv[t3, h:h + 1, :]

    for cp in sends:
        cp.wait_recv()

    y1 = layer_norm(x0r[...].astype(F32), g1[...].reshape(1, D), b1[...].reshape(1, D)).astype(BF16)
    GW = D // NG
    kv_c = []
    for g in range(NG):
        s = slice(g * GW, (g + 1) * GW)
        for j, buf in ((1, kb), (2, vb)):
            lo = j * D + g * GW
            buf[0:ROWS, s] = (dot(y1, wqkv[lo:lo + GW, :], rhs_t=True) + bq[0:1, lo:lo + GW]).astype(BF16)
        for j, buf in ((0, kb), (1, vb)):
            cp = pltpu.make_async_remote_copy(src_ref=buf.at[0:ROWS, s], dst_ref=buf.at[ROWS:2 * ROWS, s],
                                              send_sem=ks.at[2 * g + j], recv_sem=kr.at[2 * g + j],
                                              device_id={"sp": partner}, device_id_type=MESH)
            cp.start()
            kv_c.append(cp)
    for g in range(NG):
        s = slice(g * GW, (g + 1) * GW)
        qb[:, s] = (dot(y1, wqkv[g * GW:(g + 1) * GW, :], rhs_t=True) + bq[0:1, g * GW:(g + 1) * GW]).astype(BF16)

    left = lax.broadcasted_iota(jnp.int32, (ROWS, 128), 1) < HD
    osends = []
    scale = HD ** -0.5
    for g in range(NG):
        kv_c[2 * g].wait_recv()
        kv_c[2 * g + 1].wait_recv()
        for pr in range(GW // 128):
            s = slice(g * GW + pr * 128, g * GW + (pr + 1) * 128)
            q = qb[:, s]
            q2 = jnp.concatenate([jnp.where(left, q, jnp.zeros_like(q)), jnp.where(left, jnp.zeros_like(q), q)], axis=0)
            sc = dot(q2, kb[:, s], rhs_t=True) * scale
            e = jnp.exp(sc - jnp.max(sc, axis=-1, keepdims=True))
            p = (e * (1.0 / jnp.sum(e, axis=-1, keepdims=True))).astype(BF16)
            o2 = dot(p, vb[:, s])
            ob[:, s] = jnp.where(left, o2[:ROWS], o2[ROWS:]).astype(BF16)
        s = slice(g * GW, (g + 1) * GW)
        orx[0:T, s] = ob[0:T, s]
        for t in order:
            cp = pltpu.make_async_remote_copy(src_ref=ob.at[t * T:(t + 1) * T, s], dst_ref=orx.at[t * T:(t + 1) * T, s],
                                              send_sem=os_.at[g * NZ + t], recv_sem=or_.at[g * NZ + t],
                                              device_id={"sp": peer(-t)}, device_id_type=MESH)
            cp.start()
            osends.append(cp)

    for c in later_c[4:]:
        c.wait()
    res = x0h[...].astype(F32)
    n = len(order)
    for g in range(NG):
        for cp in osends[g * n:(g + 1) * n]:
            cp.wait_recv()
        s = slice(g * GW, (g + 1) * GW)
        res = res + dot(orx[:, s], wo[s, :])
    res = res + bo[...].reshape(1, D)
    y2 = layer_norm(res, g2[...].reshape(1, D), c2[...].reshape(1, D)).astype(BF16)
    acc[...] = res + bf2[...].reshape(1, D)
    FC = 768
    for f in range(FF // FC):
        s = slice(f * FC, (f + 1) * FC)
        hid = gelu_tanh(dot(y2, w1[:, s]) + bf1[...].reshape(1, FF)[:, s]).astype(BF16)
        acc[...] += dot(hid, w2[s, :])
    for t in range(NZ):
        out_ref[lax.rem(z + t, NZ)] = acc[t * T:(t + 1) * T, :].astype(BF16)

    for cp in sends + kv_c + osends:
        cp.wait_send()


def solution(mesh):
    def device_step(images, w_patch, b_patch, pos_embed, ln1_gain, ln1_bias, w_qkv, b_qkv, w_out, b_out, ln2_gain, ln2_bias, w_fc1, b_fc1, w_fc2, b_fc2):
        NB, PR, IW, C = images.shape
        PL, _, _, D = w_patch.shape
        H, HD = w_qkv.shape[2], w_qkv.shape[3]
        FF = w_fc1.shape[1]
        T = pos_embed.shape[0]
        NZ = mesh.shape["sp"] // 2
        assert NB == NZ and T == 16 and PL == 16 and IW == 256
        ROWS = NB * T
        NG = 3
        cfg = (NZ, T, PL, C, D, H, HD, FF, NG)
        vm = pltpu.VMEM
        dma = pltpu.SemaphoreType.DMA
        out = pl.pallas_call(
            functools.partial(kernel, cfg),
            out_shape=jax.ShapeDtypeStruct((NB, T, D), BF16),
            in_specs=[pl.BlockSpec(memory_space=pl.ANY)] * 16,
            out_specs=pl.BlockSpec(memory_space=pltpu.VMEM),
            scratch_shapes=[
                vm((NB, C, PL, IW), F32), vm((C, PL, 16, D), BF16), vm((D,), F32), vm((T, D), BF16),
                vm((D,), F32), vm((D,), F32), vm((3 * D, D), BF16), vm((3, H, HD), F32), vm((D, D), BF16), vm((D,), F32),
                vm((D,), F32), vm((D,), F32), vm((D, FF), BF16), vm((FF,), F32), vm((FF, D), BF16), vm((D,), F32),
                vm((C * ROWS, PL * 128), BF16), vm((PL * 128, 256), BF16), vm((ROWS, D), BF16), vm((ROWS, D), BF16),
                vm((1, 3 * D), F32), vm((ROWS, D), BF16), vm((2 * ROWS, D), BF16), vm((2 * ROWS, D), BF16),
                vm((ROWS, D), BF16), vm((ROWS, D), BF16), vm((ROWS, D), F32),
                dma((18,)), dma((NZ,)), dma((NZ,)), dma((2 * NG,)), dma((2 * NG,)), dma((NG * NZ,)), dma((NG * NZ,)),
            ],
            compiler_params=pltpu.CompilerParams(collective_id=0, has_side_effects=True, vmem_limit_bytes=60 * 1024 * 1024),
            name="siglip",
        )(
            images.transpose(0, 3, 1, 2),
            w_patch.transpose(0, 2, 1, 3),
            b_patch, pos_embed, ln1_gain, ln1_bias,
            w_qkv.transpose(1, 2, 3, 0).reshape(3 * D, D), b_qkv,
            w_out.reshape(D, D), b_out, ln2_gain, ln2_bias, w_fc1, b_fc1, w_fc2, b_fc2)
        return out

    in_specs = (P('dp', 'sp', None, None), P(), P(), P('sp', None), P(), P(), P(), P(), P(), P(), P(), P(), P(), P(), P(), P())
    return jax.shard_map(device_step, mesh=mesh, in_specs=in_specs, out_specs=P('dp', 'sp', None), check_vma=False)
```

```python
import functools
import math

import jax
import jax.numpy as jnp
from jax import lax
from jax.experimental import pallas as pl
from jax.experimental.pallas import tpu as pltpu
from jax.sharding import PartitionSpec as P

MESH = pl.DeviceIdType.MESH
LN_EPS = 1e-6
F32 = jnp.float32
BF16 = jnp.bfloat16


def dot(a, b, rhs_t=False):
    dims = (((1,), (1 if rhs_t else 0,)), ((), ()))
    return lax.dot_general(a, b, dims, preferred_element_type=F32)


def layer_norm(z, gain, bias):
    mean = jnp.mean(z, axis=-1, keepdims=True)
    centered = z - mean
    var = jnp.mean(centered * centered, axis=-1, keepdims=True)
    return centered * lax.rsqrt(var + LN_EPS) * gain + bias


def gelu_tanh(v):
    return 0.5 * v * (1.0 + jnp.tanh(math.sqrt(2.0 / math.pi) * (v + 0.044715 * (v * v * v))))


def kernel(cfg, img_hbm, wp_hbm, bp_hbm, pos_hbm, g1_hbm, b1_hbm, wqkv_hbm, bqkv_hbm, wo_hbm, bo_hbm, g2_hbm, c2_hbm,
           w1_hbm, bf1_hbm, w2_hbm, bf2_hbm, out_ref,
           img, wp, bp, pos, g1, b1, wqkv, bqkv, wo, bo, g2, c2, w1, bf1, w2, bf2,
           lhs, sel, x0h, yh, yr, wt, bq, qb, kvb, ob, orx, acc,
           dsem, isem, xs, xr, ks, kr, os_, or_):
    NZ, T, PL, C, D, H, HD, FF = cfg
    NP = D // 128
    me = lax.axis_index("sp")
    core = lax.rem(me, 2)
    z = lax.div(me, 2)
    partner = me + 1 - 2 * core
    ROWS = NZ * T

    def peer(t):
        return lax.rem(z + t + NZ, NZ) * 2 + core

    def remote(src, dst, ssem, rsem, to):
        return pltpu.make_async_remote_copy(src_ref=src, dst_ref=dst, send_sem=ssem, recv_sem=rsem,
                                            device_id={"sp": to}, device_id_type=MESH)

    barrier = pltpu.get_barrier_semaphore()
    for t in range(1, NZ):
        pl.semaphore_signal(barrier, inc=1, device_id={"sp": peer(t)}, device_id_type=MESH)
    pl.semaphore_signal(barrier, inc=1, device_id={"sp": partner}, device_id_type=MESH)

    order = sorted(range(1, NZ), key=lambda t: -min(t, NZ - t)) + [0]
    img_c = [pltpu.make_async_copy(img_hbm.at[lax.rem(z + t, NZ)], img.at[i], isem.at[i]) for i, t in enumerate(order)]
    first = [(wp_hbm.at[:, c], wp.at[c]) for c in range(C)] + [(bp_hbm, bp), (pos_hbm, pos), (g1_hbm, g1), (b1_hbm, b1)]
    later = [(wqkv_hbm, wqkv), (bqkv_hbm, bqkv), (wo_hbm, wo), (bo_hbm, bo),
             (g2_hbm, g2), (c2_hbm, c2), (w1_hbm, w1), (bf1_hbm, bf1), (w2_hbm, w2), (bf2_hbm, bf2)]
    cps = [pltpu.make_async_copy(s, d, dsem.at[i]) for i, (s, d) in enumerate(first + later)]
    first_c, later_c = cps[:len(first)], cps[len(first):]
    for c in img_c + first_c:
        c.start()

    r = lax.broadcasted_iota(jnp.int32, (256, 256), 0)
    cc = lax.broadcasted_iota(jnp.int32, (256, 256), 1)
    same_q = lax.rem(r, 16) == lax.rem(cc, 16)
    for pp in range(PL // 2):
        hit = same_q & (lax.div(cc, 16) == 2 * pp + lax.div(r, 128))
        sel[pp * 256:(pp + 1) * 256, :] = jnp.where(hit, 1.0, 0.0).astype(BF16)
    m8 = lax.div(lax.broadcasted_iota(jnp.int32, (8, 128), 1), 16) == lax.broadcasted_iota(jnp.int32, (8, 128), 0)
    GI = 2
    CH = 4
    CR = CH * T

    def spread(k):
        for i in range(CH):
            for c in range(C):
                for p in range(PL):
                    row = img[k * CH + i, c, p:p + 1, :]
                    lo = jnp.where(m8, jnp.broadcast_to(row[:, :128], (8, 128)), 0.0)
                    hi = jnp.where(m8, jnp.broadcast_to(row[:, 128:], (8, 128)), 0.0)
                    at = (((k * CH + i) // GI * C + c) * GI + i % GI) * T
                    lhs[at:at + T, p * 128:(p + 1) * 128] = jnp.concatenate([lo, hi], axis=0).astype(BF16)

    sends = []
    for k in range(NZ // CH):
        for c in img_c[k * CH:(k + 1) * CH]:
            c.wait()
        spread(k)
        xcat = []
        for u in range(CH // GI):
            at = (k * CH // GI + u) * C * GI * T
            xsel = dot(lhs[at:at + C * GI * T, :], sel[...]).astype(BF16)
            xcat.append(jnp.concatenate([xsel[c * GI * T:(c + 1) * GI * T] for c in range(C)], axis=1))
        if k == 0:
            for c in first_c:
                c.wait()
        x0 = dot(jnp.concatenate(xcat, axis=0), wp[...].reshape(C * PL * 16, D))
        posb = jnp.broadcast_to(pos[...].astype(F32)[None], (CH, T, D)).reshape(CR, D)
        x0 = (x0 + bp[...].reshape(1, D) + posb).astype(BF16)
        x0h[k * CR:(k + 1) * CR, :] = x0
        y1 = layer_norm(x0.astype(F32), g1[...].reshape(1, D), b1[...].reshape(1, D)).astype(BF16)
        yh[k * CR:(k + 1) * CR, :] = y1
        if k == NZ // CH - 1:
            yr[ROWS - T:ROWS, :] = y1[CR - T:]
        if k == 0:
            for c in later_c:
                c.start()
            pl.semaphore_wait(barrier, NZ)
        for i in range(k * CH, min((k + 1) * CH, NZ - 1)):
            cp = remote(yh.at[i * T:(i + 1) * T], yr.at[i * T:(i + 1) * T], xs.at[i], xr.at[i], peer(order[i]))
            cp.start()
            sends.append(cp)

    for c in later_c[:2]:
        c.wait()
    GW = 256
    NG = D // GW
    for n in range(3 * NP):
        j, pr = divmod(n, NP)
        to = n * 128 if j == 0 else D + pr // 2 * 2 * GW + (j - 1) * GW + pr % 2 * 128
        wt[:, to:to + 128] = wqkv[n * 128:(n + 1) * 128, :].T
        for h in range(2):
            bq[0:1, to + h * HD:to + (h + 1) * HD] = bqkv[j, 2 * pr + h:2 * pr + h + 1, :]

    for cp in sends:
        cp.wait_recv()

    y1 = yr[...]
    kv_c = []
    for g in range(NG):
        lo = D + g * 2 * GW
        sl = slice(g * 2 * GW, (g + 1) * 2 * GW)
        kvb[0:ROWS, sl] = (dot(y1, wt[:, lo:lo + 2 * GW]) + bq[0:1, lo:lo + 2 * GW]).astype(BF16)
        cp = remote(kvb.at[0:ROWS, sl], kvb.at[ROWS:2 * ROWS, sl], ks.at[g], kr.at[g], partner)
        cp.start()
        kv_c.append(cp)
    qb[...] = (dot(y1, wt[:, 0:D]) + bq[0:1, 0:D]).astype(BF16)

    left = lax.broadcasted_iota(jnp.int32, (ROWS, 128), 1) < HD
    osends = []
    scale = HD ** -0.5
    NF = 3
    for g in range(NG):
        kv_c[g].wait_recv()
        for u in range(GW // 128):
            s = slice(g * GW + u * 128, g * GW + (u + 1) * 128)
            kc = g * 2 * GW + u * 128
            q = qb[:, s]
            q2 = jnp.concatenate([jnp.where(left, q, jnp.zeros_like(q)), jnp.where(left, jnp.zeros_like(q), q)], axis=0)
            sc = dot(q2, kvb[:, kc:kc + 128], rhs_t=True) * scale
            e = jnp.exp(sc - jnp.max(sc, axis=-1, keepdims=True))
            p = (e * (1.0 / jnp.sum(e, axis=-1, keepdims=True))).astype(BF16)
            o2 = dot(p, kvb[:, kc + GW:kc + GW + 128])
            o = jnp.where(left, o2[:ROWS], o2[ROWS:]).astype(BF16)
            ob[:, s] = o
            orx[ROWS - T:ROWS, s] = o[ROWS - T:]
        s = slice(g * GW, (g + 1) * GW)
        for i in range(NF):
            n = g * NF + i
            cp = remote(ob.at[i * T:(i + 1) * T, s], orx.at[i * T:(i + 1) * T, s], os_.at[n], or_.at[n], peer(-order[i]))
            cp.start()
            osends.append(cp)
    for i in range(NF, NZ - 1):
        n = NG * NF + i - NF
        cp = remote(ob.at[i * T:(i + 1) * T], orx.at[i * T:(i + 1) * T], os_.at[n], or_.at[n], peer(-order[i]))
        cp.start()
        osends.append(cp)

    for c in later_c[2:]:
        c.wait()
    for cp in osends:
        cp.wait_recv()
    acc[...] = x0h[...].astype(F32) + bo[...].reshape(1, D) + dot(orx[...], wo[...])
    res = acc[...]
    y2 = layer_norm(res, g2[...].reshape(1, D), c2[...].reshape(1, D)).astype(BF16)
    acc[...] = res + bf2[...].reshape(1, D)
    FC = 768
    for f in range(FF // FC):
        s = slice(f * FC, (f + 1) * FC)
        hid = gelu_tanh(dot(y2, w1[:, s]) + bf1[...].reshape(1, FF)[:, s]).astype(BF16)
        acc[...] += dot(hid, w2[s, :])
    for i in range(NZ):
        out_ref[lax.rem(z + order[i], NZ)] = acc[i * T:(i + 1) * T, :].astype(BF16)

    for cp in sends + kv_c + osends:
        cp.wait_send()


def solution(mesh):
    def device_step(images, w_patch, b_patch, pos_embed, ln1_gain, ln1_bias, w_qkv, b_qkv, w_out, b_out, ln2_gain, ln2_bias, w_fc1, b_fc1, w_fc2, b_fc2):
        NB, PR, IW, C = images.shape
        PL, _, _, D = w_patch.shape
        H, HD = w_qkv.shape[2], w_qkv.shape[3]
        FF = w_fc1.shape[1]
        T = pos_embed.shape[0]
        NZ = mesh.shape["sp"] // 2
        assert NB == NZ and T == 16 and PL == 16 and IW == 256 and HD == 64
        ROWS = NB * T
        NP = D // 128
        cfg = (NZ, T, PL, C, D, H, HD, FF)
        vm = pltpu.VMEM
        dma = pltpu.SemaphoreType.DMA
        operands = (
            images.transpose(0, 3, 1, 2), w_patch.transpose(0, 2, 1, 3), b_patch, pos_embed, ln1_gain, ln1_bias,
            w_qkv.transpose(1, 2, 3, 0).reshape(3 * D, D), b_qkv, w_out.reshape(D, D), b_out, ln2_gain, ln2_bias,
            w_fc1, b_fc1, w_fc2, b_fc2)
        return pl.pallas_call(
            functools.partial(kernel, cfg),
            out_shape=jax.ShapeDtypeStruct((NB, T, D), BF16),
            in_specs=[pl.BlockSpec(memory_space=pltpu.HBM)] * len(operands),
            out_specs=pl.BlockSpec(memory_space=pltpu.VMEM),
            scratch_shapes=[
                vm((NB, C, PL, IW), F32), vm((C, PL, 16, D), BF16), vm((D,), F32), vm((T, D), BF16),
                vm((D,), F32), vm((D,), F32), vm((3 * D, D), BF16), vm((3, H, HD), F32), vm((D, D), BF16), vm((D,), F32),
                vm((D,), F32), vm((D,), F32), vm((D, FF), BF16), vm((FF,), F32), vm((FF, D), BF16), vm((D,), F32),
                vm((C * ROWS, PL * 128), BF16), vm((PL * 128, 256), BF16), vm((ROWS, D), BF16), vm((ROWS, D), BF16), vm((ROWS, D), BF16),
                vm((D, 3 * D), BF16), vm((1, 3 * D), F32), vm((ROWS, D), BF16), vm((2 * ROWS, 2 * D), BF16),
                vm((ROWS, D), BF16), vm((ROWS, D), BF16), vm((ROWS, D), F32),
                dma((17,)), dma((NZ,)), dma((NZ,)), dma((NZ,)), dma((3,)), dma((3,)), dma((3 * NZ,)), dma((3 * NZ,)),
            ],
            compiler_params=pltpu.CompilerParams(collective_id=0, has_side_effects=True, vmem_limit_bytes=40 * 1024 * 1024),
            name="siglip",
        )(*[pltpu.with_memory_space_constraint(a, pltpu.HBM) for a in operands])

    in_specs = (P('dp', 'sp', None, None), P(), P(), P('sp', None), P(), P(), P(), P(), P(), P(), P(), P(), P(), P(), P(), P())
    return jax.shard_map(device_step, mesh=mesh, in_specs=in_specs, out_specs=P('dp', 'sp', None), check_vma=False)
```
